32 devices in a mesh: rows: 4 (over y, x), cols: 8 (over z, core).
Axes of the slice: x: 2, y: 2, z: 4, core: 2. Of those that a mesh axis runs over, the one named last changes fastest.
Arguments:
- object_field: float32 [2, 1024, 2048], P(None, 'rows', 'cols'), may hold values from -6 to 6
- probe: float32 [2, 256, 256], replicated, may hold values from -6 to 6
- positions: int32 [4, 8, 6, 2], P('rows', 'cols'), may hold values from 0 to 256
- counts: int32 [4, 8], P('rows', 'cols'), may hold values from 2 to 6
- intensity: int32 [4, 8, 6, 256, 256], P('rows', 'cols'), may hold values from 0 to 4000
Outputs:
- updated_field: float32 [2, 1024, 2048], P(None, 'rows', 'cols')
The draws below stay inside these ranges and needn't reach their ends.
Inputs may be any that keep to these rules, and one draw needn't show every extreme that they name: Only the first counts[a, b] entries of tile (a, b) in positions and intensity are used.
All inputs are finite; a program needn't handle non-finite values.
Results may differ from the reference program's by a relative error of at most 0.00029.
Values sent between devices are 32-bit elements; how exact they have to be, the bound alone decides.
A program may use at most 64 MiB of HBM per device.

```python
import jax
import jax.numpy as jnp
from jax import lax

TILE = 256
MARGIN = 128
PATCH = 256
SLOTS = 6
ITERS = 2
IMG_R = 1024
IMG_C = 2048
N_ROWS = 4
N_COLS = 8


def with_ends(values, rng, low, high):
    dims = values.shape
    place = [jax.random.randint(jax.random.fold_in(rng, axis), (), 0, dims[axis]) for axis in range(len(dims))]
    values = values.at[tuple(place)].set(low)
    longest = dims.index(max(dims))
    place[longest] = (place[longest] + 1) % dims[longest]
    return values.at[tuple(place)].set(high)


def levels(rng, shape, pieces, least, high):
    def one(dim, parts):
        steps = jax.random.uniform(jax.random.fold_in(jax.random.fold_in(rng, 6), dim), (parts,), jnp.float32, least / len(pieces), high / len(pieces))
        return jnp.repeat(jnp.exp(steps), shape[dim] // parts).reshape((-1,) + (1,) * (len(shape) - dim - 1))

    loudness = one(*pieces[0])
    for cut in pieces[1:]:
        loudness = loudness * one(*cut)
    return loudness


def scatter_about(rng, extent, width, bound, split=(), kind=jnp.bfloat16):
    level = levels(rng, extent, split, -0.22, 0.18) if split else 1.0
    result = jax.random.normal(rng, extent, jnp.float32) * width * level
    return jnp.minimum(jnp.maximum(result, -bound), bound).astype(kind)


def setup_inputs(seed: int = 0) -> dict:
    keys = jax.random.split(jax.random.key(seed), 6)
    object_field = scatter_about(keys[0], (2, IMG_R, IMG_C), 1.0, 6.0, ((1, 4), (2, 8)), jnp.float32)
    probe = scatter_about(keys[1], (2, PATCH, PATCH), 1.0, 6.0, (), jnp.float32)
    positions = with_ends(jax.random.randint(keys[2], (N_ROWS, N_COLS, SLOTS, 2), 0, TILE + 2 * MARGIN - PATCH + 1), jax.random.fold_in(keys[2], 1), 0, TILE + 2 * MARGIN - PATCH).astype(jnp.int32)
    counts = with_ends(jax.random.randint(keys[3], (N_ROWS, N_COLS), 2, SLOTS + 1), jax.random.fold_in(keys[3], 1), 2, SLOTS).astype(jnp.int32)
    intensity = with_ends(jax.random.randint(keys[4], (N_ROWS, N_COLS, SLOTS, PATCH, PATCH), 0, 4001), jax.random.fold_in(keys[4], 1), 0, 4000).astype(jnp.int32)
    return {"object_field": object_field, "probe": probe, "positions": positions, "counts": counts, "intensity": intensity}


step_rate = 0.02
photon_unit = 0.001


def reference(object_field, probe, positions, counts, intensity):
    field = object_field
    probe_c = lax.complex(probe[0], probe[1])
    measured = intensity.astype(field.dtype) * photon_unit
    total = N_ROWS * N_COLS * SLOTS
    for step in range(ITERS):
        padded = jnp.pad(field, ((0, 0), (MARGIN, MARGIN), (MARGIN, MARGIN)))

        def one(item, grad):
            tile = item // SLOTS
            slot = item % SLOTS
            trow = tile // N_COLS
            tcol = tile % N_COLS
            srow = (positions[trow, tcol, slot, 0] + trow * TILE).astype(jnp.int32)
            scol = (positions[trow, tcol, slot, 1] + tcol * TILE).astype(jnp.int32)
            zero = jnp.zeros((), jnp.int32)
            patch = lax.dynamic_slice(padded, (zero, srow, scol), (2, PATCH, PATCH))
            exit_wave = probe_c * lax.complex(patch[0], patch[1])
            spectrum = jnp.fft.fft2(exit_wave, norm="ortho")
            misfit = jnp.real(spectrum) ** 2 + jnp.imag(spectrum) ** 2 - measured[trow, tcol, slot]
            back = jnp.fft.ifft2(misfit * spectrum, norm="ortho")
            term = jnp.conj(probe_c) * back
            live = (slot < counts[trow, tcol]).astype(field.dtype)
            stacked = jnp.stack([jnp.real(term), jnp.imag(term)]) * live
            old = lax.dynamic_slice(grad, (zero, srow, scol), (2, PATCH, PATCH))
            return lax.dynamic_update_slice(grad, old + stacked, (zero, srow, scol))

        grad = lax.fori_loop(0, total, one, jnp.zeros_like(padded))
        field = field - step_rate * grad[:, MARGIN:MARGIN + IMG_R, MARGIN:MARGIN + IMG_C]
    return field
```

```python
import functools

import jax
import jax.numpy as jnp
import numpy as np
from jax import lax
from jax.experimental import pallas as pl
from jax.experimental.pallas import tpu as pltpu
from jax.sharding import PartitionSpec as P

MARGIN = 128
ITERS = 2
LANES = 128
ROWS = 8


step_rate = 0.02
photon_unit = 0.001


def extended(block, sides, width):
    for axis, dim in sides:
        count = lax.axis_size(axis)
        forward = [(i, i + 1) for i in range(count - 1)]
        backward = [(target, source) for source, target in forward]
        low = lax.ppermute(
            lax.slice_in_dim(block, block.shape[dim] - width, None, axis=dim), axis, forward
        )
        high = lax.ppermute(lax.slice_in_dim(block, 0, width, axis=dim), axis, backward)
        block = jnp.concatenate([low, block, high], axis=dim)
    return block


def from_behind(block, axis, distance):
    devices = range(lax.axis_size(axis))
    route = [(i - distance, i) for i in devices if i - distance in devices]
    return lax.ppermute(block, axis, route)


def tables(length):
    half = length // 2
    k = np.arange(half)[:, None]
    n = np.arange(half)[None, :]
    found = []
    for odd in (0, 1):
        angle = ((2 * k + odd) * n % length) * (2.0 * np.pi / length)
        c = np.cos(angle) / np.sqrt(length)
        s = np.sin(angle) / np.sqrt(length)
        full = np.block([[c, s], [-s, c]])
        found += [full, full.T]
    full = np.stack(found).astype(np.float32)
    high = full.astype(jnp.bfloat16)
    low = (full - high.astype(np.float32)).astype(jnp.bfloat16)
    return np.stack([high, low])


def ordering(length):
    half = length // 2
    index = np.arange(half)
    table = np.zeros((length, length), np.float32)
    table[2 * index, index] = 1
    table[2 * index + 1, half + index] = 1
    return np.stack([table, table.T]).astype(jnp.bfloat16)


def dot(left, right):
    return lax.dot_general(left, right, (((1,), (0,)), ((), ())), preferred_element_type=jnp.float32)


def parted(value):
    high = value.astype(jnp.bfloat16)
    return high, (value - high.astype(jnp.float32)).astype(jnp.bfloat16)


def from_left(table, which, value):
    high, low = parted(value)
    return dot(table[0, which], high) + dot(table[1, which], high) + dot(table[0, which], low)


def from_right(table, which, value):
    high, low = parted(value)
    return dot(high, table[0, which]) + dot(high, table[1, which]) + dot(low, table[0, which])


def order_kernel(counts_ref, order_ref, intensity_ref, out_ref):
    @pl.loop(0, counts_ref[0, 0])
    def _(slot):
        given = intensity_ref[slot]

        def placed(value):
            value = value.astype(jnp.float32).astype(jnp.bfloat16)
            return dot(dot(order_ref[1], value).astype(jnp.bfloat16), order_ref[0])

        out_ref[slot] = (placed(given >> 4) * 16.0 + placed(given & 15)) * photon_unit


def moved_up(value, shift):
    rows, columns = value.shape
    groups = value.reshape(rows // ROWS, ROWS, columns)
    turned = pltpu.roll(groups, (ROWS - shift) % ROWS, 1)
    within = lax.broadcasted_iota(jnp.int32, (1, ROWS, columns), 1) < ROWS - shift
    return jnp.where(within, turned[:-1], turned[1:]).reshape(rows - ROWS, columns)


def moved_down(value, shift):
    rows, columns = value.shape
    groups = value.reshape(rows // ROWS, ROWS, columns)
    turned = pltpu.roll(groups, shift % ROWS, 1)
    none = jnp.zeros((1, ROWS, columns), value.dtype)
    within = lax.broadcasted_iota(jnp.int32, (1, ROWS, columns), 1) >= shift
    lower = jnp.concatenate([turned, none], axis=0)
    upper = jnp.concatenate([none, turned], axis=0)
    return jnp.where(within, lower, upper).reshape(rows + ROWS, columns)


def moved_left(value, shift):
    rows, columns = value.shape
    parts = [pltpu.roll(value[:, c : c + LANES], (LANES - shift) % LANES, 1) for c in range(0, columns, LANES)]
    within = lax.broadcasted_iota(jnp.int32, (rows, LANES), 1) < LANES - shift
    return jnp.concatenate([jnp.where(within, a, b) for a, b in zip(parts[:-1], parts[1:])], axis=1)


def moved_right(value, shift):
    rows, columns = value.shape
    parts = [pltpu.roll(value[:, c : c + LANES], shift % LANES, 1) for c in range(0, columns, LANES)]
    within = lax.broadcasted_iota(jnp.int32, (rows, LANES), 1) >= shift
    none = jnp.zeros((rows, LANES), value.dtype)
    return jnp.concatenate([jnp.where(within, a, b) for a, b in zip(parts + [none], [none] + parts)], axis=1)


def slots_kernel(positions_ref, counts_ref, padded_ref, probe_ref, measured_ref, table_ref, grad_ref):
    size = probe_ref.shape[1]
    half = size // 2
    wide = size + LANES
    last = padded_ref.shape[1] - size - ROWS
    grad_ref[...] = jnp.zeros_like(grad_ref)

    @pl.loop(0, counts_ref[0, 0])
    def _(slot):
        row = positions_ref[slot, 0]
        column = positions_ref[slot, 1]
        start = pl.multiple_of(jnp.where(column >= LANES, LANES, 0), LANES)
        shift = column - start
        first = pl.multiple_of(jnp.minimum(row // ROWS * ROWS, last), ROWS)
        drop = row - first
        there = (pl.ds(first, size + ROWS), pl.ds(start, wide))
        patch_r = moved_left(moved_up(padded_ref[(0, *there)], drop), shift)
        patch_i = moved_left(moved_up(padded_ref[(1, *there)], drop), shift)
        probe_r = probe_ref[0]
        probe_i = probe_ref[1]
        exit_r = probe_r * patch_r - probe_i * patch_i
        exit_i = probe_r * patch_i + probe_i * patch_r
        upper = jnp.concatenate([exit_r[:half], exit_i[:half]], axis=0)
        lower = jnp.concatenate([exit_r[half:], exit_i[half:]], axis=0)
        even = from_left(table_ref, 0, upper + lower)
        odd = from_left(table_ref, 2, upper - lower)
        half_r = jnp.concatenate([even[:half], odd[:half]], axis=0)
        half_i = jnp.concatenate([even[half:], odd[half:]], axis=0)
        left = jnp.concatenate([half_r[:, :half], half_i[:, :half]], axis=1)
        right = jnp.concatenate([half_r[:, half:], half_i[:, half:]], axis=1)
        backs = []
        for odd, value in ((0, left + right), (1, left - right)):
            spec = from_right(table_ref, 2 * odd + 1, value)
            spec_r, spec_i = spec[:, :half], spec[:, half:]
            misfit = spec_r * spec_r + spec_i * spec_i - measured_ref[slot, :, odd * half : (odd + 1) * half]
            scaled = jnp.concatenate([misfit * spec_r, misfit * spec_i], axis=1)
            backs.append(from_right(table_ref, 2 * odd, scaled))
        left = backs[0] + backs[1]
        right = backs[0] - backs[1]
        half_r = jnp.concatenate([left[:, :half], right[:, :half]], axis=1)
        half_i = jnp.concatenate([left[:, half:], right[:, half:]], axis=1)
        even = from_left(table_ref, 1, jnp.concatenate([half_r[:half], half_i[:half]], axis=0))
        odd = from_left(table_ref, 3, jnp.concatenate([half_r[half:], half_i[half:]], axis=0))
        upper = even + odd
        lower = even - odd
        back_r = jnp.concatenate([upper[:half], lower[:half]], axis=0)
        back_i = jnp.concatenate([upper[half:], lower[half:]], axis=0)
        term_r = probe_r * back_r + probe_i * back_i
        term_i = probe_r * back_i - probe_i * back_r
        for part, term in ((0, term_r), (1, term_i)):
            grad_ref[(part, *there)] += moved_down(moved_right(term, shift), drop)


def in_order(counts, intensity, order):
    slots, size, _ = intensity.shape
    return pl.pallas_call(
        order_kernel,
        out_shape=jax.ShapeDtypeStruct((slots, size, size), jnp.float32),
        in_specs=[pl.BlockSpec(memory_space=pltpu.SMEM)] + [pl.BlockSpec(memory_space=pltpu.VMEM)] * 2,
        out_specs=pl.BlockSpec(memory_space=pltpu.VMEM),
        cost_estimate=pl.CostEstimate(
            flops=slots * 4 * size**3, bytes_accessed=slots * 8 * size**2, transcendentals=0
        ),
        name="order",
    )(counts, order, intensity)


def slot_terms(positions, counts, padded, probe, measured, table):
    slots, size, _ = measured.shape
    return pl.pallas_call(
        slots_kernel,
        out_shape=jax.ShapeDtypeStruct(padded.shape, jnp.float32),
        in_specs=[pl.BlockSpec(memory_space=pltpu.SMEM)] * 2 + [pl.BlockSpec(memory_space=pltpu.VMEM)] * 4,
        out_specs=pl.BlockSpec(memory_space=pltpu.VMEM),
        cost_estimate=pl.CostEstimate(
            flops=slots * 48 * size**3, bytes_accessed=slots * 40 * size**2, transcendentals=0
        ),
        compiler_params=pltpu.CompilerParams(vmem_limit_bytes=48 * 1024 * 1024),
        name="slots",
    )(positions, counts, padded, probe, measured, table)


def on_device(object_field, probe, positions, counts, intensity):
    tile = object_field.shape[1]
    size = probe.shape[1]
    table = jnp.asarray(tables(size))
    order = jnp.asarray(ordering(size))
    positions = positions[0, 0]
    measured = in_order(counts, intensity[0, 0], order)
    field = object_field
    for step in range(ITERS):
        padded = extended(field, (("rows", 1), ("cols", 2)), MARGIN)
        grad = slot_terms(positions, counts, padded, probe, measured, table)
        low = MARGIN
        high = MARGIN + tile
        from_right_side = from_behind(grad[:, :, :low], "cols", -1)
        from_left_side = from_behind(grad[:, :, high:], "cols", 1)
        middle = grad[:, :, low:high]
        middle = middle.at[:, :, tile - low :].add(from_right_side)
        middle = middle.at[:, :, :low].add(from_left_side)
        from_below = from_behind(middle[:, :low, :], "rows", -1)
        from_above = from_behind(middle[:, high:, :], "rows", 1)
        owned = middle[:, low:high, :]
        owned = owned.at[:, tile - low :, :].add(from_below)
        owned = owned.at[:, :low, :].add(from_above)
        field = field - step_rate * owned
    return field


def solution(mesh):
    placed = (
        P(None, "rows", "cols"),
        P(),
        P("rows", "cols", None, None),
        P("rows", "cols"),
        P("rows", "cols", None, None, None),
    )
    return jax.shard_map(
        on_device, mesh=mesh, in_specs=placed, out_specs=P(None, "rows", "cols"), check_vma=False
    )
```

```python
import functools

import jax
import jax.numpy as jnp
import numpy as np
from jax import lax
from jax.experimental import pallas as pl
from jax.experimental.pallas import tpu as pltpu
from jax.sharding import PartitionSpec as P

MARGIN = 128
ITERS = 2
LANES = 128
ROWS = 8


step_rate = 0.02
photon_unit = 0.001


def tables(length):
    half = length // 2
    k = np.arange(half)[:, None]
    n = np.arange(half)[None, :]
    found = []
    for odd in (0, 1):
        angle = ((2 * k + odd) * n % length) * (2.0 * np.pi / length)
        c = np.cos(angle) / np.sqrt(length)
        s = np.sin(angle) / np.sqrt(length)
        full = np.block([[c, s], [-s, c]])
        found += [full, full.T]
    full = np.stack(found).astype(np.float32)
    high = full.astype(jnp.bfloat16)
    low = (full - high.astype(np.float32)).astype(jnp.bfloat16)
    return np.stack([high, low])


def ordering(length):
    half = length // 2
    index = np.arange(half)
    table = np.zeros((length, length), np.float32)
    table[2 * index, index] = 1
    table[2 * index + 1, half + index] = 1
    return np.stack([table, table.T]).astype(jnp.bfloat16)


def dot(left, right):
    return lax.dot_general(left, right, (((1,), (0,)), ((), ())), preferred_element_type=jnp.float32)


def parted(value):
    high = value.astype(jnp.bfloat16)
    return high, (value - high.astype(jnp.float32)).astype(jnp.bfloat16)


def from_left(table, which, value):
    high, low = parted(value)
    return dot(table[0, which], high) + dot(table[1, which], high) + dot(table[0, which], low)


def from_right(table, which, value):
    high, low = parted(value)
    return dot(high, table[0, which]) + dot(high, table[1, which]) + dot(low, table[0, which])


def order_kernel(counts_ref, order_ref, intensity_ref, out_ref):
    @pl.loop(0, counts_ref[0, 0])
    def _(slot):
        given = intensity_ref[slot]

        def placed(value):
            value = value.astype(jnp.float32).astype(jnp.bfloat16)
            return dot(dot(order_ref[1], value).astype(jnp.bfloat16), order_ref[0])

        out_ref[slot] = (placed(given >> 4) * 16.0 + placed(given & 15)) * photon_unit


def moved_up(value, shift):
    rows, columns = value.shape
    groups = value.reshape(rows // ROWS, ROWS, columns)
    turned = pltpu.roll(groups, (ROWS - shift) % ROWS, 1)
    within = lax.broadcasted_iota(jnp.int32, (1, ROWS, columns), 1) < ROWS - shift
    return jnp.where(within, turned[:-1], turned[1:]).reshape(rows - ROWS, columns)


def moved_down(value, shift):
    rows, columns = value.shape
    groups = value.reshape(rows // ROWS, ROWS, columns)
    turned = pltpu.roll(groups, shift % ROWS, 1)
    none = jnp.zeros((1, ROWS, columns), value.dtype)
    within = lax.broadcasted_iota(jnp.int32, (1, ROWS, columns), 1) >= shift
    lower = jnp.concatenate([turned, none], axis=0)
    upper = jnp.concatenate([none, turned], axis=0)
    return jnp.where(within, lower, upper).reshape(rows + ROWS, columns)


def moved_left(value, shift):
    rows, columns = value.shape
    parts = [pltpu.roll(value[:, c : c + LANES], (LANES - shift) % LANES, 1) for c in range(0, columns, LANES)]
    within = lax.broadcasted_iota(jnp.int32, (rows, LANES), 1) < LANES - shift
    return jnp.concatenate([jnp.where(within, a, b) for a, b in zip(parts[:-1], parts[1:])], axis=1)


def moved_right(value, shift):
    rows, columns = value.shape
    parts = [pltpu.roll(value[:, c : c + LANES], shift % LANES, 1) for c in range(0, columns, LANES)]
    within = lax.broadcasted_iota(jnp.int32, (rows, LANES), 1) >= shift
    none = jnp.zeros((rows, LANES), value.dtype)
    return jnp.concatenate([jnp.where(within, a, b) for a, b in zip(parts + [none], [none] + parts)], axis=1)


def slots_kernel(positions_ref, counts_ref, padded_ref, probe_ref, measured_ref, table_ref, grad_ref):
    size = probe_ref.shape[1]
    half = size // 2
    wide = size + LANES
    last = padded_ref.shape[1] - size - ROWS
    grad_ref[...] = jnp.zeros_like(grad_ref)

    @pl.loop(0, counts_ref[0, 0])
    def _(slot):
        row = positions_ref[slot, 0]
        column = positions_ref[slot, 1]
        start = pl.multiple_of(jnp.where(column >= LANES, LANES, 0), LANES)
        shift = column - start
        first = pl.multiple_of(jnp.minimum(row // ROWS * ROWS, last), ROWS)
        drop = row - first
        there = (pl.ds(first, size + ROWS), pl.ds(start, wide))
        patch_r = moved_left(moved_up(padded_ref[(0, *there)], drop), shift)
        patch_i = moved_left(moved_up(padded_ref[(1, *there)], drop), shift)
        probe_r = probe_ref[0]
        probe_i = probe_ref[1]
        exit_r = probe_r * patch_r - probe_i * patch_i
        exit_i = probe_r * patch_i + probe_i * patch_r
        upper = jnp.concatenate([exit_r[:half], exit_i[:half]], axis=0)
        lower = jnp.concatenate([exit_r[half:], exit_i[half:]], axis=0)
        even = from_left(table_ref, 0, upper + lower)
        odd = from_left(table_ref, 2, upper - lower)
        half_r = jnp.concatenate([even[:half], odd[:half]], axis=0)
        half_i = jnp.concatenate([even[half:], odd[half:]], axis=0)
        left = jnp.concatenate([half_r[:, :half], half_i[:, :half]], axis=1)
        right = jnp.concatenate([half_r[:, half:], half_i[:, half:]], axis=1)
        backs = []
        for odd, value in ((0, left + right), (1, left - right)):
            spec = from_right(table_ref, 2 * odd + 1, value)
            spec_r, spec_i = spec[:, :half], spec[:, half:]
            misfit = spec_r * spec_r + spec_i * spec_i - measured_ref[slot, :, odd * half : (odd + 1) * half]
            scaled = jnp.concatenate([misfit * spec_r, misfit * spec_i], axis=1)
            backs.append(from_right(table_ref, 2 * odd, scaled))
        left = backs[0] + backs[1]
        right = backs[0] - backs[1]
        half_r = jnp.concatenate([left[:, :half], right[:, :half]], axis=1)
        half_i = jnp.concatenate([left[:, half:], right[:, half:]], axis=1)
        even = from_left(table_ref, 1, jnp.concatenate([half_r[:half], half_i[:half]], axis=0))
        odd = from_left(table_ref, 3, jnp.concatenate([half_r[half:], half_i[half:]], axis=0))
        upper = even + odd
        lower = even - odd
        back_r = jnp.concatenate([upper[:half], lower[:half]], axis=0)
        back_i = jnp.concatenate([upper[half:], lower[half:]], axis=0)
        term_r = probe_r * back_r + probe_i * back_i
        term_i = probe_r * back_i - probe_i * back_r
        for part, term in ((0, term_r), (1, term_i)):
            grad_ref[(part, *there)] += moved_down(moved_right(term, shift), drop)


def in_order(counts, intensity, order):
    slots, size, _ = intensity.shape
    return pl.pallas_call(
        order_kernel,
        out_shape=jax.ShapeDtypeStruct((slots, size, size), jnp.float32),
        in_specs=[pl.BlockSpec(memory_space=pltpu.SMEM)] + [pl.BlockSpec(memory_space=pltpu.VMEM)] * 2,
        out_specs=pl.BlockSpec(memory_space=pltpu.VMEM),
        cost_estimate=pl.CostEstimate(
            flops=slots * 4 * size**3, bytes_accessed=slots * 8 * size**2, transcendentals=0
        ),
        name="order",
    )(counts, order, intensity)


def slot_terms(positions, counts, padded, probe, measured, table):
    slots, size, _ = measured.shape
    return pl.pallas_call(
        slots_kernel,
        out_shape=jax.ShapeDtypeStruct(padded.shape, jnp.float32),
        in_specs=[pl.BlockSpec(memory_space=pltpu.SMEM)] * 2 + [pl.BlockSpec(memory_space=pltpu.VMEM)] * 4,
        out_specs=pl.BlockSpec(memory_space=pltpu.VMEM),
        cost_estimate=pl.CostEstimate(
            flops=slots * 48 * size**3, bytes_accessed=slots * 40 * size**2, transcendentals=0
        ),
        compiler_params=pltpu.CompilerParams(vmem_limit_bytes=48 * 1024 * 1024),
        name="slots",
    )(positions, counts, padded, probe, measured, table)


MESH = pl.DeviceIdType.MESH


class Around:
    def __init__(self, send_sems, recv_sems):
        self.send_sems, self.recv_sems = send_sems, recv_sems
        self.here, self.device = {}, {}
        for axis in ("rows", "cols"):
            count = lax.axis_size(axis)
            me = lax.axis_index(axis)
            self.here[axis, -1], self.here[axis, 1] = me > 0, me < count - 1
            self.device[axis, -1] = {axis: lax.rem(me + count - 1, count)}
            self.device[axis, 1] = {axis: lax.rem(me + 1, count)}

    def meet(self):
        barrier = pltpu.get_barrier_semaphore()
        for side, there in self.here.items():

            @pl.when(there)
            def _():
                pl.semaphore_signal(barrier, inc=1, device_id=self.device[side], device_id_type=MESH)

        pl.semaphore_wait(barrier, sum(there.astype(jnp.int32) for there in self.here.values()))

    def copy(self, index, side, source, target):
        return pltpu.make_async_remote_copy(
            src_ref=source,
            dst_ref=target,
            send_sem=self.send_sems.at[index],
            recv_sem=self.recv_sems.at[index],
            device_id=self.device[side],
            device_id_type=MESH,
        )


def both(first, second):
    return jnp.logical_and(first, second)


def no(flag):
    return jnp.logical_not(flag)


def pad_kernel(field_ref, out_ref, send_sems, recv_sems):
    m = MARGIN
    planes, high, wide = field_ref.shape
    around = Around(send_sems, recv_sems)
    here = around.here
    around.meet()
    row_cuts = {-1: (pl.ds(0, m), pl.ds(m + high, m)), 1: (pl.ds(high - m, m), pl.ds(0, m))}
    col_cuts = {-1: (pl.ds(0, m), pl.ds(m + wide, m)), 1: (pl.ds(wide - m, m), pl.ds(0, m))}
    from_cuts = {-1: pl.ds(0, m), 1: pl.ds(m + high, m)}
    col_from = {-1: pl.ds(m, m), 1: pl.ds(wide, m)}
    rows, cols, corners = {}, {}, {}
    index = 0
    for p in range(planes):
        for d in (-1, 1):
            cut, land = row_cuts[d]
            rows[p, d] = around.copy(
                index, ("rows", d), field_ref.at[p, cut, :], out_ref.at[p, land, pl.ds(m, wide)]
            )
            cut, land = col_cuts[d]
            cols[p, d] = around.copy(
                index + 1, ("cols", d), field_ref.at[p, :, cut], out_ref.at[p, pl.ds(m, high), land]
            )
            index += 2
            for v in (-1, 1):
                corners[p, v, d] = around.copy(
                    index, ("cols", d), out_ref.at[p, from_cuts[v], col_from[d]], out_ref.at[p, from_cuts[v], land]
                )
                index += 1
    for p in range(planes):
        for d in (-1, 1):
            pl.when(here["rows", d])(rows[p, d].start)
    for p in range(planes):
        for d in (-1, 1):
            pl.when(here["cols", d])(cols[p, d].start)
    out_ref[:, m : m + high, m : m + wide] = field_ref[...]
    for v in (-1, 1):

        @pl.when(no(here["rows", v]))
        def _():
            out_ref[:, from_cuts[v], m : m + wide] = jnp.zeros((planes, m, wide), jnp.float32)

        for d in (-1, 1):
            land = col_cuts[-d][1]

            @pl.when(no(both(here["rows", v], here["cols", d])))
            def _():
                out_ref[:, from_cuts[v], land] = jnp.zeros((planes, m, m), jnp.float32)

    for d in (-1, 1):
        land = col_cuts[-d][1]

        @pl.when(no(here["cols", d]))
        def _():
            out_ref[:, m : m + high, land] = jnp.zeros((planes, high, m), jnp.float32)

    for p in range(planes):
        for v in (-1, 1):
            pl.when(here["rows", v])(rows[p, -v].wait_recv)
            for d in (-1, 1):
                pl.when(both(here["rows", v], here["cols", d]))(corners[p, v, d].start)
    for p in range(planes):
        for d in (-1, 1):
            pl.when(here["cols", d])(cols[p, -d].wait_recv)
            for v in (-1, 1):
                pl.when(both(here["rows", v], here["cols", d]))(corners[p, v, -d].wait_recv)
    for p in range(planes):
        for d in (-1, 1):
            pl.when(here["rows", d])(rows[p, d].wait_send)
            pl.when(here["cols", d])(cols[p, d].wait_send)
            for v in (-1, 1):
                pl.when(both(here["rows", v], here["cols", d]))(corners[p, v, d].wait_send)


def step_kernel(last, grad_ref, padded_ref, out_ref, mid_ref, side_ref, band_ref, send_sems, recv_sems):
    m = MARGIN
    planes, extent, _ = grad_ref.shape
    tall = extent // 2
    wide = extent - 2 * m
    around = Around(send_sems, recv_sems)
    here = around.here
    around.meet()
    chains = [(p, h) for p in range(planes) for h in (-1, 1)]
    halves = {-1: pl.ds(0, tall), 1: pl.ds(tall, tall)}
    own = {-1: pl.ds(m, tall - m), 1: pl.ds(tall, tall - m)}
    sides, bands, edges = {}, {}, {}
    index = 0
    cut = {-1: pl.ds(0, m), 1: pl.ds(extent - m, m)}
    inner = {-1: pl.ds(m, m), 1: pl.ds(wide, m)}
    for p, h in chains:
        for d in (-1, 1):
            slot = (d + 1) // 2
            sides[p, h, d] = around.copy(
                index, ("cols", d), grad_ref.at[p, halves[h], cut[d]], side_ref.at[slot, p, halves[h]]
            )
            index += 1
            if not last:
                edges[p, h, d] = around.copy(
                    index, ("cols", d), out_ref.at[p, halves[h], inner[d]], out_ref.at[p, halves[h], cut[-d]]
                )
                index += 1
        if last:
            goes, lands = cut[h], own[-h]
        else:
            goes, lands = halves[h], halves[-h]
        bands[p, h] = around.copy(index, ("rows", h), mid_ref.at[p, goes], band_ref.at[p, lands])
        index += 1
    for p, h in chains:
        for d in (-1, 1):
            pl.when(here["cols", d])(sides[p, h, d].start)
    if not last:
        for d in (-1, 1):

            @pl.when(no(here["cols", d]))
            def _():
                out_ref[:, :, cut[d]] = jnp.zeros((planes, extent, m), jnp.float32)

    for p, h in chains:
        mid_ref[p, halves[h]] = grad_ref[p, halves[h], m : m + wide]
        for d in (-1, 1):
            slot = (1 - d) // 2
            target = pl.ds(0, m) if d < 0 else pl.ds(wide - m, m)

            @pl.when(here["cols", d])
            def _():
                sides[p, h, -d].wait_recv()
                mid_ref[p, halves[h], target] += side_ref[slot, p, halves[h]]

        pl.when(here["rows", h])(bands[p, h].start)
    for p, h in chains:
        whole = own[h] if last else halves[h]

        @pl.when(here["rows", h])
        def _():
            bands[p, -h].wait_recv()
            total = mid_ref[p, whole] + band_ref[p, whole]
            value = padded_ref[p, whole, m : m + wide] - step_rate * total
            if last:
                out_ref[p, pl.ds(own[h].start - m, tall - m)] = value
            else:
                out_ref[p, whole, m : m + wide] = value

        @pl.when(no(here["rows", h]))
        def _():
            value = padded_ref[p, own[h], m : m + wide] - step_rate * mid_ref[p, own[h]]
            if last:
                out_ref[p, pl.ds(own[h].start - m, tall - m)] = value
            else:
                out_ref[p, own[h], m : m + wide] = value
                out_ref[p, cut[h], m : m + wide] = jnp.zeros((m, wide), jnp.float32)

        if not last:
            for d in (-1, 1):
                pl.when(here["cols", d])(edges[p, h, d].start)
    for p, h in chains:
        for d in (-1, 1):
            if not last:
                pl.when(here["cols", d])(edges[p, h, -d].wait_recv)
                pl.when(here["cols", d])(edges[p, h, d].wait_send)
            pl.when(here["cols", d])(sides[p, h, d].wait_send)
        pl.when(here["rows", h])(bands[p, h].wait_send)


def exchange(kernel, name, collective_id, shape, scratch, copies, *arrays):
    return pl.pallas_call(
        kernel,
        out_shape=jax.ShapeDtypeStruct(shape, jnp.float32),
        in_specs=[pl.BlockSpec(memory_space=pltpu.VMEM)] * len(arrays),
        out_specs=pl.BlockSpec(memory_space=pltpu.VMEM),
        scratch_shapes=[pltpu.VMEM(s, jnp.float32) for s in scratch]
        + [pltpu.SemaphoreType.DMA((copies,)), pltpu.SemaphoreType.DMA((copies,))],
        compiler_params=pltpu.CompilerParams(
            collective_id=collective_id, has_side_effects=True, vmem_limit_bytes=32 * 1024 * 1024
        ),
        name=name,
    )(*arrays)


def on_device(object_field, probe, positions, counts, intensity):
    planes, high, wide = object_field.shape
    size = probe.shape[1]
    table = jnp.asarray(tables(size))
    order = jnp.asarray(ordering(size))
    positions = positions[0, 0]
    measured = in_order(counts, intensity[0, 0], order)
    tall, broad = high + 2 * MARGIN, wide + 2 * MARGIN
    outer = (planes, tall, broad)
    scratch = [(planes, tall, wide), (2, planes, tall, MARGIN), (planes, tall, wide)]
    padded = exchange(pad_kernel, "pad", 0, outer, [], 8 * planes, object_field)
    for step in range(ITERS):
        grad = slot_terms(positions, counts, padded, probe, measured, table)
        last = step == ITERS - 1
        kernel = functools.partial(step_kernel, last)
        shape = object_field.shape if last else outer
        padded = exchange(kernel, "step", 1 + step, shape, scratch, 10 * planes, grad, padded)
    return padded


def solution(mesh):
    placed = (
        P(None, "rows", "cols"),
        P(),
        P("rows", "cols", None, None),
        P("rows", "cols"),
        P("rows", "cols", None, None, None),
    )
    return jax.shard_map(
        on_device, mesh=mesh, in_specs=placed, out_specs=P(None, "rows", "cols"), check_vma=False
    )
```

```python
import functools

import jax
import jax.numpy as jnp
import numpy as np
from jax import lax
from jax.experimental import pallas as pl
from jax.experimental.pallas import tpu as pltpu
from jax.sharding import PartitionSpec as P

MARGIN = 128
ITERS = 2
LANES = 128
ROWS = 8


step_rate = 0.02
photon_unit = 0.001


def tables(length):
    half = length // 2
    k = np.arange(half)[:, None]
    n = np.arange(half)[None, :]
    found = []
    for odd in (0, 1):
        angle = ((2 * k + odd) * n % length) * (2.0 * np.pi / length)
        c = np.cos(angle) / np.sqrt(length)
        s = np.sin(angle) / np.sqrt(length)
        full = np.block([[c, s], [-s, c]])
        found += [full, full.T]
    full = np.stack(found).astype(np.float32)
    high = full.astype(jnp.bfloat16)
    low = (full - high.astype(np.float32)).astype(jnp.bfloat16)
    return np.stack([high, low])


def ordering(length):
    half = length // 2
    index = np.arange(half)
    table = np.zeros((length, length), np.float32)
    table[2 * index, index] = 1
    table[2 * index + 1, half + index] = 1
    return np.stack([table, table.T]).astype(jnp.bfloat16)


def dot(left, right):
    return lax.dot_general(left, right, (((1,), (0,)), ((), ())), preferred_element_type=jnp.float32)


def parted(value):
    high = value.astype(jnp.bfloat16)
    return high, (value - high.astype(jnp.float32)).astype(jnp.bfloat16)


def from_left(table, which, value):
    high, low = parted(value)
    return dot(table[0, which], high) + dot(table[1, which], high) + dot(table[0, which], low)


def from_right(table, which, value):
    high, low = parted(value)
    return dot(high, table[0, which]) + dot(high, table[1, which]) + dot(low, table[0, which])


def order_kernel(counts_ref, order_ref, intensity_ref, out_ref):
    @pl.loop(0, counts_ref[0, 0])
    def _(slot):
        given = intensity_ref[slot]

        def placed(value):
            value = value.astype(jnp.float32).astype(jnp.bfloat16)
            return dot(dot(order_ref[1], value).astype(jnp.bfloat16), order_ref[0])

        out_ref[slot] = (placed(given >> 4) * 16.0 + placed(given & 15)) * photon_unit


def moved_up(value, shift):
    rows, columns = value.shape
    groups = value.reshape(rows // ROWS, ROWS, columns)
    turned = pltpu.roll(groups, (ROWS - shift) % ROWS, 1)
    within = lax.broadcasted_iota(jnp.int32, (1, ROWS, columns), 1) < ROWS - shift
    return jnp.where(within, turned[:-1], turned[1:]).reshape(rows - ROWS, columns)


def moved_down(value, shift):
    rows, columns = value.shape
    groups = value.reshape(rows // ROWS, ROWS, columns)
    turned = pltpu.roll(groups, shift % ROWS, 1)
    none = jnp.zeros((1, ROWS, columns), value.dtype)
    within = lax.broadcasted_iota(jnp.int32, (1, ROWS, columns), 1) >= shift
    lower = jnp.concatenate([turned, none], axis=0)
    upper = jnp.concatenate([none, turned], axis=0)
    return jnp.where(within, lower, upper).reshape(rows + ROWS, columns)


def moved_left(value, shift):
    rows, columns = value.shape
    parts = [pltpu.roll(value[:, c : c + LANES], (LANES - shift) % LANES, 1) for c in range(0, columns, LANES)]
    within = lax.broadcasted_iota(jnp.int32, (rows, LANES), 1) < LANES - shift
    return jnp.concatenate([jnp.where(within, a, b) for a, b in zip(parts[:-1], parts[1:])], axis=1)


def moved_right(value, shift):
    rows, columns = value.shape
    parts = [pltpu.roll(value[:, c : c + LANES], shift % LANES, 1) for c in range(0, columns, LANES)]
    within = lax.broadcasted_iota(jnp.int32, (rows, LANES), 1) >= shift
    none = jnp.zeros((rows, LANES), value.dtype)
    return jnp.concatenate([jnp.where(within, a, b) for a, b in zip(parts + [none], [none] + parts)], axis=1)


def slots_kernel(positions_ref, counts_ref, padded_ref, probe_ref, measured_ref, table_ref, grad_ref):
    size = probe_ref.shape[1]
    half = size // 2
    wide = size + LANES
    last = padded_ref.shape[1] - size - ROWS
    grad_ref[...] = jnp.zeros_like(grad_ref)

    @pl.loop(0, counts_ref[0, 0])
    def _(slot):
        row = positions_ref[slot, 0]
        column = positions_ref[slot, 1]
        start = pl.multiple_of(jnp.where(column >= LANES, LANES, 0), LANES)
        shift = column - start
        first = pl.multiple_of(jnp.minimum(row // ROWS * ROWS, last), ROWS)
        drop = row - first
        there = (pl.ds(first, size + ROWS), pl.ds(start, wide))
        patch_r = moved_left(moved_up(padded_ref[(0, *there)], drop), shift)
        patch_i = moved_left(moved_up(padded_ref[(1, *there)], drop), shift)
        probe_r = probe_ref[0]
        probe_i = probe_ref[1]
        exit_r = probe_r * patch_r - probe_i * patch_i
        exit_i = probe_r * patch_i + probe_i * patch_r
        upper = jnp.concatenate([exit_r[:half], exit_i[:half]], axis=0)
        lower = jnp.concatenate([exit_r[half:], exit_i[half:]], axis=0)
        even = from_left(table_ref, 0, upper + lower)
        odd = from_left(table_ref, 2, upper - lower)
        half_r = jnp.concatenate([even[:half], odd[:half]], axis=0)
        half_i = jnp.concatenate([even[half:], odd[half:]], axis=0)
        left = jnp.concatenate([half_r[:, :half], half_i[:, :half]], axis=1)
        right = jnp.concatenate([half_r[:, half:], half_i[:, half:]], axis=1)
        backs = []
        for odd, value in ((0, left + right), (1, left - right)):
            spec = from_right(table_ref, 2 * odd + 1, value)
            spec_r, spec_i = spec[:, :half], spec[:, half:]
            misfit = spec_r * spec_r + spec_i * spec_i - measured_ref[slot, :, odd * half : (odd + 1) * half]
            scaled = jnp.concatenate([misfit * spec_r, misfit * spec_i], axis=1)
            backs.append(from_right(table_ref, 2 * odd, scaled))
        left = backs[0] + backs[1]
        right = backs[0] - backs[1]
        half_r = jnp.concatenate([left[:, :half], right[:, :half]], axis=1)
        half_i = jnp.concatenate([left[:, half:], right[:, half:]], axis=1)
        even = from_left(table_ref, 1, jnp.concatenate([half_r[:half], half_i[:half]], axis=0))
        odd = from_left(table_ref, 3, jnp.concatenate([half_r[half:], half_i[half:]], axis=0))
        upper = even + odd
        lower = even - odd
        back_r = jnp.concatenate([upper[:half], lower[:half]], axis=0)
        back_i = jnp.concatenate([upper[half:], lower[half:]], axis=0)
        term_r = probe_r * back_r + probe_i * back_i
        term_i = probe_r * back_i - probe_i * back_r
        for part, term in ((0, term_r), (1, term_i)):
            grad_ref[(part, *there)] += moved_down(moved_right(term, shift), drop)


def in_order(counts, intensity, order):
    slots, size, _ = intensity.shape
    return pl.pallas_call(
        order_kernel,
        out_shape=jax.ShapeDtypeStruct((slots, size, size), jnp.float32),
        in_specs=[pl.BlockSpec(memory_space=pltpu.SMEM)] + [pl.BlockSpec(memory_space=pltpu.VMEM)] * 2,
        out_specs=pl.BlockSpec(memory_space=pltpu.VMEM),
        cost_estimate=pl.CostEstimate(
            flops=slots * 4 * size**3, bytes_accessed=slots * 8 * size**2, transcendentals=0
        ),
        compiler_params=pltpu.CompilerParams(vmem_limit_bytes=12 * 1024 * 1024),
        name="order",
    )(counts, order, intensity)


def slot_terms(positions, counts, padded, probe, measured, table):
    slots, size, _ = measured.shape
    return pl.pallas_call(
        slots_kernel,
        out_shape=jax.ShapeDtypeStruct(padded.shape, jnp.float32),
        in_specs=[pl.BlockSpec(memory_space=pltpu.SMEM)] * 2 + [pl.BlockSpec(memory_space=pltpu.VMEM)] * 4,
        out_specs=pl.BlockSpec(memory_space=pltpu.VMEM),
        cost_estimate=pl.CostEstimate(
            flops=slots * 48 * size**3, bytes_accessed=slots * 40 * size**2, transcendentals=0
        ),
        compiler_params=pltpu.CompilerParams(vmem_limit_bytes=20 * 1024 * 1024),
        name="slots",
    )(positions, counts, padded, probe, measured, table)


MESH = pl.DeviceIdType.MESH


class Around:
    def __init__(self, send_sems, recv_sems):
        self.send_sems, self.recv_sems = send_sems, recv_sems
        self.here, self.device = {}, {}
        for axis in ("rows", "cols"):
            count = lax.axis_size(axis)
            me = lax.axis_index(axis)
            self.here[axis, -1], self.here[axis, 1] = me > 0, me < count - 1
            self.device[axis, -1] = {axis: lax.rem(me + count - 1, count)}
            self.device[axis, 1] = {axis: lax.rem(me + 1, count)}

    def meet(self):
        barrier = pltpu.get_barrier_semaphore()
        for side, there in self.here.items():

            @pl.when(there)
            def _():
                pl.semaphore_signal(barrier, inc=1, device_id=self.device[side], device_id_type=MESH)

        pl.semaphore_wait(barrier, sum(there.astype(jnp.int32) for there in self.here.values()))

    def copy(self, index, side, source, target):
        return pltpu.make_async_remote_copy(
            src_ref=source,
            dst_ref=target,
            send_sem=self.send_sems.at[index],
            recv_sem=self.recv_sems.at[index],
            device_id=self.device[side],
            device_id_type=MESH,
        )


def both(first, second):
    return jnp.logical_and(first, second)


def no(flag):
    return jnp.logical_not(flag)


def pad_kernel(field_ref, out_ref, send_sems, recv_sems):
    m = MARGIN
    planes, high, wide = field_ref.shape
    around = Around(send_sems, recv_sems)
    here = around.here
    around.meet()
    row_cuts = {-1: (pl.ds(0, m), pl.ds(m + high, m)), 1: (pl.ds(high - m, m), pl.ds(0, m))}
    col_cuts = {-1: (pl.ds(0, m), pl.ds(m + wide, m)), 1: (pl.ds(wide - m, m), pl.ds(0, m))}
    from_cuts = {-1: pl.ds(0, m), 1: pl.ds(m + high, m)}
    col_from = {-1: pl.ds(m, m), 1: pl.ds(wide, m)}
    rows, cols, corners = {}, {}, {}
    index = 0
    for p in range(planes):
        for d in (-1, 1):
            cut, land = row_cuts[d]
            rows[p, d] = around.copy(
                index, ("rows", d), field_ref.at[p, cut, :], out_ref.at[p, land, pl.ds(m, wide)]
            )
            cut, land = col_cuts[d]
            cols[p, d] = around.copy(
                index + 1, ("cols", d), field_ref.at[p, :, cut], out_ref.at[p, pl.ds(m, high), land]
            )
            index += 2
            for v in (-1, 1):
                corners[p, v, d] = around.copy(
                    index, ("cols", d), out_ref.at[p, from_cuts[v], col_from[d]], out_ref.at[p, from_cuts[v], land]
                )
                index += 1
    for p in range(planes):
        for d in (-1, 1):
            pl.when(here["rows", d])(rows[p, d].start)
    for p in range(planes):
        for d in (-1, 1):
            pl.when(here["cols", d])(cols[p, d].start)
    out_ref[:, m : m + high, m : m + wide] = field_ref[...]
    for v in (-1, 1):

        @pl.when(no(here["rows", v]))
        def _():
            out_ref[:, from_cuts[v], m : m + wide] = jnp.zeros((planes, m, wide), jnp.float32)

        for d in (-1, 1):
            land = col_cuts[-d][1]

            @pl.when(no(both(here["rows", v], here["cols", d])))
            def _():
                out_ref[:, from_cuts[v], land] = jnp.zeros((planes, m, m), jnp.float32)

    for d in (-1, 1):
        land = col_cuts[-d][1]

        @pl.when(no(here["cols", d]))
        def _():
            out_ref[:, m : m + high, land] = jnp.zeros((planes, high, m), jnp.float32)

    for p in range(planes):
        for v in (-1, 1):
            pl.when(here["rows", v])(rows[p, -v].wait_recv)
            for d in (-1, 1):
                pl.when(both(here["rows", v], here["cols", d]))(corners[p, v, d].start)
    for p in range(planes):
        for d in (-1, 1):
            pl.when(here["cols", d])(cols[p, -d].wait_recv)
            for v in (-1, 1):
                pl.when(both(here["rows", v], here["cols", d]))(corners[p, v, -d].wait_recv)
    for p in range(planes):
        for d in (-1, 1):
            pl.when(here["rows", d])(rows[p, d].wait_send)
            pl.when(here["cols", d])(cols[p, d].wait_send)
            for v in (-1, 1):
                pl.when(both(here["rows", v], here["cols", d]))(corners[p, v, d].wait_send)


def step_kernel(last, grad_ref, padded_ref, out_ref, mid_ref, side_ref, band_ref, send_sems, recv_sems):
    m = MARGIN
    planes, extent, _ = grad_ref.shape
    tall = extent // 2
    wide = extent - 2 * m
    around = Around(send_sems, recv_sems)
    here = around.here
    around.meet()
    chains = [(p, h) for p in range(planes) for h in (-1, 1)]
    halves = {-1: pl.ds(0, tall), 1: pl.ds(tall, tall)}
    own = {-1: pl.ds(m, tall - m), 1: pl.ds(tall, tall - m)}
    sides, bands, edges = {}, {}, {}
    index = 0
    cut = {-1: pl.ds(0, m), 1: pl.ds(extent - m, m)}
    inner = {-1: pl.ds(m, m), 1: pl.ds(wide, m)}
    for p, h in chains:
        for d in (-1, 1):
            slot = (d + 1) // 2
            sides[p, h, d] = around.copy(
                index, ("cols", d), grad_ref.at[p, halves[h], cut[d]], side_ref.at[slot, p, halves[h]]
            )
            index += 1
            if not last:
                edges[p, h, d] = around.copy(
                    index, ("cols", d), out_ref.at[p, halves[h], inner[d]], out_ref.at[p, halves[h], cut[-d]]
                )
                index += 1
        if last:
            goes, lands = cut[h], own[-h]
        else:
            goes, lands = halves[h], halves[-h]
        bands[p, h] = around.copy(index, ("rows", h), mid_ref.at[p, goes], band_ref.at[p, lands])
        index += 1
    for p, h in chains:
        for d in (-1, 1):
            pl.when(here["cols", d])(sides[p, h, d].start)
    if not last:
        for d in (-1, 1):

            @pl.when(no(here["cols", d]))
            def _():
                out_ref[:, :, cut[d]] = jnp.zeros((planes, extent, m), jnp.float32)

    for p, h in chains:
        mid_ref[p, halves[h]] = grad_ref[p, halves[h], m : m + wide]
        for d in (-1, 1):
            slot = (1 - d) // 2
            target = pl.ds(0, m) if d < 0 else pl.ds(wide - m, m)

            @pl.when(here["cols", d])
            def _():
                sides[p, h, -d].wait_recv()
                mid_ref[p, halves[h], target] += side_ref[slot, p, halves[h]]

        pl.when(here["rows", h])(bands[p, h].start)
    for p, h in chains:
        whole = own[h] if last else halves[h]

        @pl.when(here["rows", h])
        def _():
            bands[p, -h].wait_recv()
            total = mid_ref[p, whole] + band_ref[p, whole]
            value = padded_ref[p, whole, m : m + wide] - step_rate * total
            if last:
                out_ref[p, pl.ds(own[h].start - m, tall - m)] = value
            else:
                out_ref[p, whole, m : m + wide] = value

        @pl.when(no(here["rows", h]))
        def _():
            value = padded_ref[p, own[h], m : m + wide] - step_rate * mid_ref[p, own[h]]
            if last:
                out_ref[p, pl.ds(own[h].start - m, tall - m)] = value
            else:
                out_ref[p, own[h], m : m + wide] = value
                out_ref[p, cut[h], m : m + wide] = jnp.zeros((m, wide), jnp.float32)

        if not last:
            for d in (-1, 1):
                pl.when(here["cols", d])(edges[p, h, d].start)
    for p, h in chains:
        for d in (-1, 1):
            if not last:
                pl.when(here["cols", d])(edges[p, h, -d].wait_recv)
                pl.when(here["cols", d])(edges[p, h, d].wait_send)
            pl.when(here["cols", d])(sides[p, h, d].wait_send)
        pl.when(here["rows", h])(bands[p, h].wait_send)


def exchange(kernel, name, collective_id, shape, scratch, copies, *arrays):
    return pl.pallas_call(
        kernel,
        out_shape=jax.ShapeDtypeStruct(shape, jnp.float32),
        in_specs=[pl.BlockSpec(memory_space=pltpu.VMEM)] * len(arrays),
        out_specs=pl.BlockSpec(memory_space=pltpu.VMEM),
        scratch_shapes=[pltpu.VMEM(s, jnp.float32) for s in scratch]
        + [pltpu.SemaphoreType.DMA((copies,)), pltpu.SemaphoreType.DMA((copies,))],
        compiler_params=pltpu.CompilerParams(
            collective_id=collective_id, has_side_effects=True, vmem_limit_bytes=12 * 1024 * 1024
        ),
        name=name,
    )(*arrays)


def on_device(object_field, probe, positions, counts, intensity):
    planes, high, wide = object_field.shape
    size = probe.shape[1]
    table = jnp.asarray(tables(size))
    order = jnp.asarray(ordering(size))
    positions = positions[0, 0]
    measured = in_order(counts, intensity[0, 0], order)
    tall, broad = high + 2 * MARGIN, wide + 2 * MARGIN
    outer = (planes, tall, broad)
    scratch = [(planes, tall, wide), (2, planes, tall, MARGIN), (planes, tall, wide)]
    padded = exchange(pad_kernel, "pad", 0, outer, [], 8 * planes, object_field)
    for step in range(ITERS):
        grad = slot_terms(positions, counts, padded, probe, measured, table)
        last = step == ITERS - 1
        kernel = functools.partial(step_kernel, last)
        shape = object_field.shape if last else outer
        padded = exchange(kernel, "step", 1 + step, shape, scratch, 10 * planes, grad, padded)
    return padded


def solution(mesh):
    placed = (
        P(None, "rows", "cols"),
        P(),
        P("rows", "cols", None, None),
        P("rows", "cols"),
        P("rows", "cols", None, None, None),
    )
    return jax.shard_map(
        on_device, mesh=mesh, in_specs=placed, out_specs=P(None, "rows", "cols"), check_vma=False
    )
```
